32 devices in a mesh: ens: 2 (over y), hist: 4 (over z), mom: 2 (over x), rep: 2 (over core).
Axes of the slice: x: 2, y: 2, z: 4, core: 2. Of those that a mesh axis runs over, the one named last changes fastest.
Arguments:
- history_stat: float32 [512, 1024, 512], P(('hist', 'rep'), 'ens', 'mom'), parts along dimension 1, may hold values from -6 to 6, as said below
- history_spec: float32 [512, 1024, 512], P(('hist', 'rep'), 'ens', 'mom'), parts along dimension 1, may hold values from -6 to 6, as said below
Outputs:
- rows_stat: float32 [6, 512, 512], P('ens', ('hist', 'rep'), 'mom'), parts along dimension 0
- rows_spec: float32 [6, 512, 512], P('ens', ('hist', 'rep'), 'mom'), parts along dimension 0
- newest_stat: float32 [10, 5, 512], P('ens', None, 'mom'), parts along dimension 0
- newest_spec: float32 [10, 5, 512], P('ens', None, 'mom'), parts along dimension 0
The draws below stay inside these ranges and needn't reach their ends.
There are 2 independent parts, one for each index of `ens`. The reference program is written for one: setup_inputs(seed, part) draws one part's arguments, and reference() takes and returns one part's arrays. A program takes and returns all parts, laid end to end along the dimension named above; each array names one. Nothing has to cross between parts.
Inputs may be any that keep to these rules, and one draw needn't show every extreme that they name: `history_stat`: symmetric under exchange of its two time indices. `history_spec`: antisymmetric under exchange of its two time indices, zero where they are equal.
All inputs are finite; a program needn't handle non-finite values.
Results may differ from the reference program's by a relative error of at most 0.0003.
Values sent between devices are 32-bit elements; how exact they have to be, the bound alone decides.
No kernel may reach another device: no remote copies, remote signals or barrier semaphores. Data moves between devices by JAX's collectives and lax.ppermute only.
A program may use at most 128 MiB of HBM per device.

```python
import math
import jax
import jax.numpy as jnp
from jax import lax

TIMES = 512
MOMENTA = 512
STEPS = 3


def clipped_base(key, salt):
    base = jax.random.normal(jax.random.fold_in(key, salt), (TIMES, TIMES, MOMENTA), jnp.float32)
    return jnp.clip(base, -6.0, 6.0)


def draw_history_stat(key, part):
    base = clipped_base(key, 11)
    field = 0.5 * (base + jnp.transpose(base, (1, 0, 2)))
    return field


def draw_history_spec(key, part):
    base = clipped_base(key, 17)
    field = 0.5 * (base - jnp.transpose(base, (1, 0, 2)))
    return field


def setup_inputs(seed: int = 0, part: int = 0) -> dict:
    key_list = jax.random.split(jax.random.key(seed), 3)
    own_keys = jax.random.split(jax.random.fold_in(key_list[2], part), 3)
    history_stat = draw_history_stat(jax.random.fold_in(jax.random.fold_in(key_list[2], part), 71), part)
    history_spec = draw_history_spec(jax.random.fold_in(jax.random.fold_in(key_list[2], part), 71), part)
    return dict(history_stat=history_stat, history_spec=history_spec)


TIME_STEP = 0.12
CUTOFF = 12.8
MASS_SQUARED = 1.0
SUNSET_COUPLING = 100.0
HARTREE_COUPLING = 2.45
HIGHEST = lax.Precision.HIGHEST


def sine_values(left_index, right_index, points):
    product = ((left_index[:, None] + 1) * (right_index[None, :] + 1)) % (2 * (points + 1))
    return jnp.sin(product.astype(jnp.float32) * (math.pi / (points + 1)))


def forward_table(momentum_index, radius_index, points):
    momentum_step = CUTOFF / points
    radius_step = math.pi / ((points + 1) * momentum_step)
    momentum = (momentum_index.astype(jnp.float32) + 1.0) * momentum_step
    radius = (radius_index.astype(jnp.float32) + 1.0) * radius_step
    return sine_values(momentum_index, radius_index, points) * (momentum[:, None] * momentum_step) / (2.0 * math.pi ** 2 * radius[None, :])


def backward_table(radius_index, momentum_index, points):
    momentum_step = CUTOFF / points
    radius_step = math.pi / ((points + 1) * momentum_step)
    momentum = (momentum_index.astype(jnp.float32) + 1.0) * momentum_step
    radius = (radius_index.astype(jnp.float32) + 1.0) * radius_step
    return sine_values(radius_index, momentum_index, points) * (4.0 * math.pi * radius_step * radius[:, None]) / momentum[None, :]


def sunset(field_stat, field_spec):
    square_stat = field_stat * field_stat
    square_spec = field_spec * field_spec
    sigma_stat = -SUNSET_COUPLING * field_stat * (square_stat - 0.75 * square_spec)
    sigma_spec = -SUNSET_COUPLING * field_spec * (3.0 * square_stat - 0.25 * square_spec)
    return sigma_stat, sigma_spec


def reference(history_stat, history_spec):
    time_count = TIMES
    row_count = TIMES
    newest = STEPS + 2
    momentum_step = CUTOFF / MOMENTA
    row_times = jnp.arange(row_count, dtype=jnp.int32)
    column_times = jnp.arange(time_count, dtype=jnp.int32)
    newest_times = time_count - 2 + jnp.arange(newest, dtype=jnp.int32)
    newest_index = jnp.arange(newest, dtype=jnp.int32)
    later_mask = (row_times[:, None] <= column_times[None, :]).astype(jnp.float32)
    earlier_mask = (row_times[:, None] >= column_times[None, :]).astype(jnp.float32)
    newest_later = (row_times[:, None] <= newest_times[None, :]).astype(jnp.float32)
    newest_earlier = (row_times[:, None] >= newest_times[None, :]).astype(jnp.float32)
    upper_pairs = (newest_index[:, None] <= newest_index[None, :]).astype(jnp.float32)
    lower_pairs = (newest_index[:, None] >= newest_index[None, :]).astype(jnp.float32)
    every_index = jnp.arange(MOMENTA, dtype=jnp.int32)
    momentum = (every_index.astype(jnp.float32) + 1.0) * momentum_step
    measure = momentum * momentum * momentum_step / (2.0 * math.pi ** 2)
    forward = forward_table(every_index, every_index, MOMENTA)
    backward = backward_table(every_index, every_index, MOMENTA)
    block_stat = jnp.zeros((newest, newest, MOMENTA), jnp.float32).at[:2, :2].set(history_stat[time_count - 2:, time_count - 2:, :])
    block_spec = jnp.zeros((newest, newest, MOMENTA), jnp.float32).at[:2, :2].set(history_spec[time_count - 2:, time_count - 2:, :])
    column_stat = jnp.zeros((newest, row_count, MOMENTA), jnp.float32).at[:2].set(jnp.transpose(history_stat[:, time_count - 2:, :], (1, 0, 2)))
    column_spec = jnp.zeros((newest, row_count, MOMENTA), jnp.float32).at[:2].set(-jnp.transpose(history_spec[:, time_count - 2:, :], (1, 0, 2)))
    factor = TIME_STEP * TIME_STEP
    for step_index in range(STEPS):
        current = step_index + 1
        stack_stat = jnp.concatenate([column_stat[current], block_stat[current]], axis=0)
        stack_spec = jnp.concatenate([column_spec[current], block_spec[current]], axis=0)
        tadpole = jnp.sum(measure * block_stat[current, current])
        radial_stat = jnp.dot(stack_stat, forward, precision=HIGHEST)
        radial_spec = jnp.dot(stack_spec, forward, precision=HIGHEST)
        sigma_stat, sigma_spec = sunset(radial_stat, radial_spec)
        sigma_stat = jnp.dot(sigma_stat, backward, precision=HIGHEST)
        sigma_spec = jnp.dot(sigma_spec, backward, precision=HIGHEST)
        group_stat, newest_sstat = sigma_stat[:row_count], sigma_stat[row_count:]
        group_spec, newest_sspec = sigma_spec[:row_count], sigma_spec[row_count:]
        memory_stat = jnp.einsum("ip,it,itp->tp", group_stat, later_mask, history_spec, precision=HIGHEST) - jnp.einsum("ip,itp->tp", group_spec, history_stat, precision=HIGHEST)
        memory_spec = -jnp.einsum("ip,it,itp->tp", group_spec, earlier_mask, history_spec, precision=HIGHEST)
        newest_mstat = -jnp.einsum("ip,aip->ap", group_spec, column_stat, precision=HIGHEST) - jnp.einsum("ip,ia,aip->ap", group_stat, newest_later, column_spec, precision=HIGHEST)
        newest_mspec = jnp.einsum("ip,ia,aip->ap", group_spec, newest_earlier, column_spec, precision=HIGHEST)
        active = ((newest_index >= 2) & (newest_index <= current)).astype(jnp.float32)[:, None]
        weight_spec = newest_sspec * active
        weight_stat = newest_sstat * active
        memory_stat = memory_stat - jnp.einsum("bp,bip->ip", weight_spec, column_stat, precision=HIGHEST)
        memory_spec = memory_spec - jnp.einsum("bp,bip->ip", weight_spec, column_spec, precision=HIGHEST)
        newest_mstat = newest_mstat - jnp.einsum("bp,bap->ap", weight_spec, block_stat, precision=HIGHEST) + jnp.einsum("bp,ba,bap->ap", weight_stat, upper_pairs, block_spec, precision=HIGHEST)
        newest_mspec = newest_mspec - jnp.einsum("bp,ba,bap->ap", weight_spec, lower_pairs, block_spec, precision=HIGHEST)
        frequency = momentum * momentum + MASS_SQUARED + HARTREE_COUPLING * tadpole
        next_stat = 2.0 * column_stat[current] - column_stat[step_index] - factor * (frequency * column_stat[current] + TIME_STEP * memory_stat)
        next_spec = 2.0 * column_spec[current] - column_spec[step_index] - factor * (frequency * column_spec[current] + TIME_STEP * memory_spec)
        column_stat = column_stat.at[current + 1].set(next_stat)
        column_spec = column_spec.at[current + 1].set(next_spec)
        valid_mask = (newest_index <= current).astype(jnp.float32)[:, None]
        line_stat = valid_mask * (2.0 * block_stat[current] - block_stat[step_index] - factor * (frequency * block_stat[current] + TIME_STEP * newest_mstat))
        line_spec = valid_mask * (2.0 * block_spec[current] - block_spec[step_index] - factor * (frequency * block_spec[current] + TIME_STEP * newest_mspec))
        diagonal = 2.0 * line_stat[current] - line_stat[step_index] - factor * (frequency * line_stat[current] + TIME_STEP * newest_mstat[current])
        line_stat = line_stat.at[current + 1].set(diagonal)
        block_stat = block_stat.at[current + 1].set(line_stat).at[:, current + 1].set(line_stat)
        block_spec = block_spec.at[current + 1].set(line_spec).at[:, current + 1].set(-line_spec)
    return column_stat[2:], column_spec[2:], block_stat, block_spec
```

```python
import functools
import math

import jax
import jax.numpy as jnp
import numpy as np
from jax import lax
from jax.experimental import pallas as pl
from jax.experimental.pallas import tpu as pltpu
from jax.sharding import PartitionSpec as P

MOMENTA = 512
STEPS = 3
TIME_STEP = 0.12
CUTOFF = 12.8
MASS_SQUARED = 1.0
SUNSET_COUPLING = 100.0
HARTREE_COUPLING = 2.45
HIGHEST = lax.Precision.HIGHEST

SUB = 8
LANES = 128
WIDE = 32
RESIDENT_BYTES = 40 * 2**20
PART_ROWS = 16
EXTRA = 32
F32 = jnp.float32
VMEM = pl.BlockSpec(memory_space=pltpu.VMEM)
HBM = pl.BlockSpec(memory_space=pltpu.HBM)
SMEM = pl.BlockSpec(memory_space=pltpu.SMEM)


def params(mib):
    return pltpu.CompilerParams(vmem_limit_bytes=mib * 2**20)


def tables(points):
    index = np.arange(points, dtype=np.int64) + 1
    momentum_step = CUTOFF / points
    radius_step = math.pi / ((points + 1) * momentum_step)
    sine = np.sin((index[:, None] * index[None, :]) % (2 * (points + 1)) * (math.pi / (points + 1)))
    momentum = index * momentum_step
    radius = index * radius_step
    forward = sine * (momentum[:, None] * momentum_step) / (2.0 * math.pi**2 * radius[None, :])
    backward = sine * (4.0 * math.pi * radius_step * radius[:, None]) / momentum[None, :]
    measure = momentum * momentum * momentum_step / (2.0 * math.pi**2)
    return tuple(np.asarray(a, np.float32) for a in (forward, backward, measure, momentum))


def shifts(size, amount):
    return [(i, (i + amount) % size) for i in range(size)]


def first_kernel(stat_hbm, spec_hbm, c0, c1, d0, d1, out_ref, stat_ref, spec_ref, sem):
    rows, _, width = stat_ref.shape
    latest = pl.ds(stat_hbm.shape[1] - SUB, SUB)
    copies = [
        pltpu.make_async_copy(stat_hbm.at[:, latest], stat_ref, sem.at[0]),
        pltpu.make_async_copy(spec_hbm.at[:, latest], spec_ref, sem.at[1]),
    ]
    for c in copies:
        c.start()
    for c in copies:
        c.wait()
    c0[...] = stat_ref[:, SUB - 2, :]
    c1[...] = stat_ref[:, SUB - 1, :]
    d0[...] = -spec_ref[:, SUB - 2, :]
    d1[...] = -spec_ref[:, SUB - 1, :]
    half = rows + SUB
    out_ref[0:rows, :] = c1[...]
    out_ref[half : half + rows, :] = d1[...]
    out_ref[rows:half, :] = jnp.zeros((SUB, width), F32)
    out_ref[half + rows :, :] = jnp.zeros((SUB, width), F32)


def load_kernel(counts, *refs):
    n = len(counts)
    sources, outs, sem = refs[:n], refs[n + 1 : 2 * n + 1], refs[-1]
    copies = [
        pltpu.make_async_copy(sources[i].at[pl.ds(start, count)], outs[i], sem.at[i])
        for i, (start, count) in enumerate(counts)
    ]
    for c in copies:
        c.start()
    for c in copies:
        c.wait()


def load(sources, counts, order):
    return pl.pallas_call(
        functools.partial(load_kernel, counts),
        out_shape=[pltpu.VMEM((n,) + s.shape[1:], F32) for s, (_, n) in zip(sources, counts)],
        in_specs=[HBM] * len(sources) + [VMEM],
        out_specs=[VMEM] * len(sources),
        scratch_shapes=[pltpu.SemaphoreType.DMA((len(sources),))],
        compiler_params=params(2),
        name="load",
    )(*sources, order)


def transform_kernel(step, blocks, *refs):
    current = step + 1
    place = refs[0]
    pieces = refs[1 : 1 + blocks]
    forward, backward, measure = refs[1 + blocks : 4 + blocks]
    stats = refs[4 + blocks : 5 + blocks + current]
    specs = refs[5 + blocks + current : 6 + blocks + 2 * current]
    out_ref, own_ref = refs[6 + blocks + 2 * current :]
    rows, width = stats[0].shape
    half = rows + SUB
    own = place[0]
    times = place[1] * rows
    radial = None
    tadpole = None
    for k in range(blocks):
        block = lax.rem(own + (blocks - k), blocks)
        part = jnp.dot(pieces[k][...], forward[block], precision=HIGHEST, preferred_element_type=F32)
        radial = part if radial is None else radial + part
        line = rows - 1 if step == 0 else rows + current
        part = jnp.sum(pieces[k][line : line + 1, :] * measure[block], axis=1, keepdims=True)
        tadpole = part if tadpole is None else tadpole + part
    stat = radial[:half]
    spec = radial[half:]
    square_stat = stat * stat
    square_spec = spec * spec
    sigma_stat = -SUNSET_COUPLING * stat * (square_stat - 0.75 * square_spec)
    sigma_spec = -SUNSET_COUPLING * spec * (3.0 * square_stat - 0.25 * square_spec)
    sigma = jnp.concatenate([sigma_stat, sigma_spec], axis=0)
    sigma = jnp.dot(sigma, backward[own], precision=HIGHEST, preferred_element_type=F32)
    group_stat = sigma[:rows]
    group_spec = sigma[half : half + rows]
    out_ref[0:rows, :] = group_stat
    out_ref[rows : 2 * rows, :] = group_spec
    own_ref[0:SUB, :] = sigma[rows:half]
    own_ref[SUB : 2 * SUB, :] = sigma[half + rows :]
    row_times = times + lax.broadcasted_iota(jnp.int32, (rows, width), 0)
    index = lax.broadcasted_iota(jnp.int32, (SUB, width), 0)
    base = 2 * rows
    sums_stat = jnp.zeros((SUB, width), F32)
    sums_spec = jnp.zeros((SUB, width), F32)
    last = place[2]
    for a in range(current + 1):
        column_stat = stats[a][...]
        column_spec = specs[a][...]
        later = row_times <= last - 1 + a
        earlier = row_times >= last - 1 + a
        partial = -group_spec * column_stat - jnp.where(later, group_stat * column_spec, 0.0)
        sums_stat = jnp.where(index == a, jnp.sum(partial, axis=0, keepdims=True), sums_stat)
        partial = jnp.where(earlier, group_spec * column_spec, 0.0)
        sums_spec = jnp.where(index == a, jnp.sum(partial, axis=0, keepdims=True), sums_spec)
    out_ref[base : base + SUB, :] = sums_stat
    out_ref[base + SUB : base + 2 * SUB, :] = sums_spec
    out_ref[base + 2 * SUB : base + 3 * SUB, :] = jnp.concatenate(
        [r[rows - 2 : rows, :] for r in (stats[0], stats[1], specs[0], specs[1])], axis=0
    )
    out_ref[base + 3 * SUB :, :] = jnp.broadcast_to(tadpole, (SUB, width))


def memory_kernel(step, group_sizes, resident, stream, *refs):
    current = step + 1
    newest = STEPS + 2
    hists, reps = group_sizes
    groups = hists * reps
    refs = list(refs)

    def take(n):
        head = refs[:n]
        del refs[:n]
        return head

    (place,) = take(1)
    pieces = take(groups)
    (own_ref, momentum) = take(2)
    stats = take(current + 1)
    specs = take(current + 1)
    blocks_in = take(2) if step else None
    stat_parts = take(len(resident[0]))
    spec_parts = take(len(resident[1]))
    hbm = take(1) if stream else None
    last_step = step == STEPS - 1
    if last_step:
        rows_stat, rows_spec, block_stat, block_spec = take(4)
    else:
        next_stat_ref, next_spec_ref, block_stat, block_spec, out_ref = take(5)
    sig_stat, sig_spec, extra, mem_stat, mem_spec = take(5)
    if stream:
        buffers, sem = take(2)
    rows, width = stats[0].shape
    times = groups * rows
    hist, rep = place[3], place[4]
    group = hist * reps + rep
    chunks = rows // SUB

    def copy(c):
        slot = (c - stream[0]) % 2
        return pltpu.make_async_copy(hbm[0].at[pl.ds(c * SUB, SUB)], buffers.at[slot], sem.at[slot])

    if stream:
        for c in range(stream[0], min(stream[0] + 2, chunks)):
            copy(c).start()
    for k in range(hists):
        for q in range(reps):
            piece = pieces[k * reps + q]
            who = lax.rem(hist + (hists - k), hists) * reps + lax.rem(rep + (reps - q), reps)
            at = pl.multiple_of(who * rows, SUB)
            sig_stat[pl.ds(at, rows), :] = piece[0:rows, :]
            sig_spec[pl.ds(at, rows), :] = piece[rows : 2 * rows, :]
            extra[who] = piece[2 * rows :, :]

    def find(parts, sizes, c):
        start = c * SUB
        for ref, (first, count) in zip(parts, sizes):
            if first <= start < first + count:
                return ref, start - first
        return None, 0

    tile = lax.broadcasted_iota(jnp.int32, (SUB, LANES), 0)
    for c in range(chunks):
        stat_ref, stat_at = find(stat_parts, resident[0], c)
        spec_ref, spec_at = find(spec_parts, resident[1], c)
        if spec_ref is None:
            copy(c).wait()
            spec_ref, spec_at = buffers.at[(c - stream[0]) % 2], 0
        first_time = group * rows + c * SUB
        middle = first_time // WIDE
        for l in range(width // LANES):
            lane = slice(l * LANES, (l + 1) * LANES)

            def below(j, acc, stat_ref=stat_ref, stat_at=stat_at, spec_ref=spec_ref, spec_at=spec_at, lane=lane):
                acc_stat, acc_spec = list(acc[0]), list(acc[1])
                for t in range(WIDE // SUB):
                    at = pl.ds(pl.multiple_of(j * WIDE + t * SUB, SUB), SUB)
                    weight_stat, weight_spec = sig_stat[at, lane], sig_spec[at, lane]
                    for r in range(SUB):
                        acc_stat[r] += weight_spec * stat_ref[stat_at + r, at, lane]
                        acc_stat[r] += weight_stat * spec_ref[spec_at + r, at, lane]
                return tuple(acc_stat), tuple(acc_spec)

            def above(j, acc, stat_ref=stat_ref, stat_at=stat_at, spec_ref=spec_ref, spec_at=spec_at, lane=lane):
                acc_stat, acc_spec = list(acc[0]), list(acc[1])
                for t in range(WIDE // SUB):
                    at = pl.ds(pl.multiple_of(j * WIDE + t * SUB, SUB), SUB)
                    weight_spec = sig_spec[at, lane]
                    for r in range(SUB):
                        acc_stat[r] += weight_spec * stat_ref[stat_at + r, at, lane]
                        acc_spec[r] += weight_spec * spec_ref[spec_at + r, at, lane]
                return tuple(acc_stat), tuple(acc_spec)

            zero = jnp.zeros((SUB, LANES), F32)
            acc = (tuple(zero for _ in range(SUB)), tuple(zero for _ in range(SUB)))
            acc = lax.fori_loop(0, middle, below, acc)
            acc_stat, acc_spec = list(acc[0]), list(acc[1])
            for t in range(WIDE // SUB):
                start = pl.multiple_of(middle * WIDE + t * SUB, SUB)
                at = pl.ds(start, SUB)
                weight_stat, weight_spec = sig_stat[at, lane], sig_spec[at, lane]
                for r in range(SUB):
                    value = spec_ref[spec_at + r, at, lane]
                    early = start + tile <= first_time + r
                    acc_stat[r] += weight_spec * stat_ref[stat_at + r, at, lane]
                    acc_stat[r] += jnp.where(early, weight_stat * value, 0.0)
                    acc_spec[r] += jnp.where(early, 0.0, weight_spec * value)
            acc = (tuple(acc_stat), tuple(acc_spec))
            acc = lax.fori_loop(middle + 1, times // WIDE, above, acc)
            mem_stat[c * SUB : (c + 1) * SUB, lane] = -jnp.concatenate(
                [jnp.sum(a, axis=0, keepdims=True) for a in acc[0]], axis=0
            )
            mem_spec[c * SUB : (c + 1) * SUB, lane] = jnp.concatenate(
                [jnp.sum(a, axis=0, keepdims=True) for a in acc[1]], axis=0
            )
        if stream and c >= stream[0] and c + 2 < chunks:
            copy(c + 2).start()

    factor = TIME_STEP * TIME_STEP
    corner = extra[groups - 1]
    index = lax.broadcasted_iota(jnp.int32, (SUB, width), 0)
    zero = jnp.zeros((SUB, width), F32)
    if step == 0:
        def pick(first, sign):
            out = []
            for a in range(2):
                left = corner[2 * SUB + first + a : 2 * SUB + first + a + 1, :]
                right = corner[2 * SUB + first + 2 + a : 2 * SUB + first + 3 + a, :]
                out.append(jnp.where(index == 0, sign * left, jnp.where(index == 1, sign * right, 0.0)))
            return out + [zero] * (newest - 2)

        blk_stat = pick(0, 1.0)
        blk_spec = pick(4, -1.0)
    else:
        blk_stat = [blocks_in[0][b] for b in range(newest)]
        blk_spec = [blocks_in[1][b] for b in range(newest)]
    tadpole = corner[3 * SUB : 3 * SUB + 1, :]
    momentum = momentum[place[0]]
    frequency = momentum * momentum + MASS_SQUARED + HARTREE_COUPLING * tadpole

    total_stat = extra[0, 0:SUB, :]
    total_spec = extra[0, SUB : 2 * SUB, :]
    for g in range(1, groups):
        total_stat += extra[g, 0:SUB, :]
        total_spec += extra[g, SUB : 2 * SUB, :]
    memory_stat = mem_stat[...]
    memory_spec = mem_spec[...]
    for b in range(2, current + 1):
        weight_stat = own_ref[b : b + 1, :]
        weight_spec = own_ref[SUB + b : SUB + b + 1, :]
        memory_stat -= weight_spec * stats[b][...]
        memory_spec -= weight_spec * specs[b][...]
        total_stat -= weight_spec * blk_stat[b]
        total_stat += jnp.where(index >= b, weight_stat * blk_spec[b], 0.0)
        total_spec -= jnp.where(index <= b, weight_spec * blk_spec[b], 0.0)
    new_stat = (
        2.0 * stats[current][...]
        - stats[step][...]
        - factor * (frequency * stats[current][...] + TIME_STEP * memory_stat)
    )
    new_spec = (
        2.0 * specs[current][...]
        - specs[step][...]
        - factor * (frequency * specs[current][...] + TIME_STEP * memory_spec)
    )
    valid = index <= current
    line_stat = jnp.where(
        valid,
        2.0 * blk_stat[current]
        - blk_stat[step]
        - factor * (frequency * blk_stat[current] + TIME_STEP * total_stat),
        0.0,
    )
    line_spec = jnp.where(
        valid,
        2.0 * blk_spec[current]
        - blk_spec[step]
        - factor * (frequency * blk_spec[current] + TIME_STEP * total_spec),
        0.0,
    )
    diagonal = (
        2.0 * line_stat[current : current + 1]
        - line_stat[step : step + 1]
        - factor
        * (frequency * line_stat[current : current + 1] + TIME_STEP * total_stat[current : current + 1])
    )
    line_stat = jnp.where(index == current + 1, diagonal, line_stat)
    blk_stat[current + 1] = line_stat
    blk_spec[current + 1] = line_spec
    for b in range(newest):
        block_stat[b] = jnp.where(index == current + 1, line_stat[b : b + 1], blk_stat[b])
        block_spec[b] = jnp.where(index == current + 1, -line_spec[b : b + 1], blk_spec[b])
    if last_step:
        for b in range(2, newest - 1):
            rows_stat[b - 2] = stats[b][...]
            rows_spec[b - 2] = specs[b][...]
        rows_stat[newest - 3] = new_stat
        rows_spec[newest - 3] = new_spec
    else:
        next_stat_ref[...] = new_stat
        next_spec_ref[...] = new_spec
        half = rows + SUB
        out_ref[0:rows, :] = new_stat
        out_ref[half : half + rows, :] = new_spec
        out_ref[rows:half, :] = line_stat
        out_ref[half + rows :, :] = line_spec


def shards(history_stat, history_spec):
    rows, times, width = history_stat.shape
    history_stat = pltpu.with_memory_space_constraint(history_stat, pltpu.HBM)
    history_spec = pltpu.with_memory_space_constraint(history_spec, pltpu.HBM)
    newest = STEPS + 2
    half = rows + SUB
    hists, reps, moms = (lax.axis_size(a) for a in ("hist", "rep", "mom"))
    forward, backward, measure, momentum = tables(MOMENTA)
    forward = jnp.asarray(forward.reshape(moms, width, MOMENTA))
    backward = jnp.asarray(np.ascontiguousarray(backward.reshape(MOMENTA, moms, width).transpose(1, 0, 2)))
    measure = jnp.asarray(measure.reshape(moms, 1, width))
    own = lax.axis_index("mom")
    hist, rep = lax.axis_index("hist"), lax.axis_index("rep")
    momentum = jnp.asarray(momentum.reshape(moms, 1, width))
    place = jnp.stack([own, hist * reps + rep, jnp.int32(times - 1), hist, rep]).astype(jnp.int32)

    row_bytes = times * width * 4
    keep = min(2 * rows, RESIDENT_BYTES // row_bytes // SUB * SUB)
    keep_stat = rows
    keep_spec = keep - rows
    split = PART_ROWS
    sizes_stat = [(r, min(split, keep_stat - r)) for r in range(0, keep_stat, split)]
    sizes_spec = [(r, min(split, keep_spec - r)) for r in range(0, keep_spec, split)]
    stream = (keep_spec // SUB,) if keep_spec < rows else None

    c0, c1, d0, d1, send = pl.pallas_call(
        first_kernel,
        in_specs=[HBM] * 2,
        out_specs=[VMEM] * 5,
        out_shape=[jax.ShapeDtypeStruct((rows, width), F32)] * 4
        + [jax.ShapeDtypeStruct((2 * half, width), F32)],
        scratch_shapes=[pltpu.VMEM((rows, SUB, width), F32)] * 2 + [pltpu.SemaphoreType.DMA((2,))],
        compiler_params=params(3),
        name="first",
    )(history_stat, history_spec)
    stats, specs = [c0, c1], [d0, d1]
    blocks = ()
    for step in range(STEPS):
        pieces = [send] + [lax.ppermute(send, "mom", shifts(moms, k)) for k in range(1, moms)]
        z, own_rows = pl.pallas_call(
            functools.partial(transform_kernel, step, moms),
            in_specs=[SMEM] + [VMEM] * (moms + 3 + len(stats) + len(specs)),
            out_specs=[VMEM] * 2,
            out_shape=[
                jax.ShapeDtypeStruct((2 * rows + EXTRA, width), F32),
                jax.ShapeDtypeStruct((2 * SUB, width), F32),
            ],
            compiler_params=params(6),
            name=f"transform_{step}",
        )(place, *pieces, forward, backward, measure, *stats, *specs)
        along = [z] + [lax.ppermute(z, "hist", shifts(hists, k)) for k in range(1, hists)]
        if step == 0:
            sources = [history_stat] * len(sizes_stat) + [history_spec] * len(sizes_spec)
            kept = [load([a], [n], z)[0] for a, n in zip(sources, sizes_stat + sizes_spec)]
        gathered = []
        for piece in along:
            gathered += [piece] + [lax.ppermute(piece, "rep", shifts(reps, q)) for q in range(1, reps)]
        last = step == STEPS - 1
        block_shape = jax.ShapeDtypeStruct((newest, SUB, width), F32)
        row_shape = jax.ShapeDtypeStruct((rows, width), F32)
        if last:
            out_shape = [jax.ShapeDtypeStruct((STEPS, rows, width), F32)] * 2 + [block_shape] * 2
        else:
            out_shape = [row_shape] * 2 + [block_shape] * 2
            out_shape += [jax.ShapeDtypeStruct((2 * half, width), F32)]
        scratch = [pltpu.VMEM((times, width), F32)] * 2 + [
            pltpu.VMEM((hists * reps, EXTRA, width), F32),
            pltpu.VMEM((rows, width), F32),
            pltpu.VMEM((rows, width), F32),
        ]
        operands = [*gathered, own_rows, momentum, *stats, *specs, *blocks, *kept]
        in_specs = [SMEM] + [VMEM] * len(operands)
        if stream:
            operands.append(history_spec)
            in_specs.append(HBM)
            scratch += [pltpu.VMEM((2, SUB, times, width), F32), pltpu.SemaphoreType.DMA((2,))]
        outs = pl.pallas_call(
            functools.partial(
                memory_kernel, step, (hists, reps), (sizes_stat, sizes_spec), stream
            ),
            in_specs=in_specs,
            out_specs=[VMEM] * len(out_shape),
            out_shape=out_shape,
            scratch_shapes=scratch,
            compiler_params=params(11),
            name=f"memory_{step}",
        )(place, *operands)
        if last:
            return outs[0], outs[1], outs[2][:, :newest], outs[3][:, :newest]
        stats.append(outs[0])
        specs.append(outs[1])
        blocks = (outs[2], outs[3])
        send = outs[4]


def solution(mesh):
    in_specs = (P(("hist", "rep"), "ens", "mom"), P(("hist", "rep"), "ens", "mom"))
    out_specs = (
        P("ens", ("hist", "rep"), "mom"),
        P("ens", ("hist", "rep"), "mom"),
        P("ens", None, "mom"),
        P("ens", None, "mom"),
    )
    return jax.shard_map(shards, mesh=mesh, in_specs=in_specs, out_specs=out_specs, check_vma=False)
```

```python
import functools
import math

import jax
import jax.numpy as jnp
import numpy as np
from jax import lax
from jax.experimental import pallas as pl
from jax.experimental.pallas import tpu as pltpu
from jax.sharding import PartitionSpec as P


MOMENTA = 512
STEPS = 3
TIME_STEP = 0.12
CUTOFF = 12.8
MASS_SQUARED = 1.0
SUNSET_COUPLING = 100.0
HARTREE_COUPLING = 2.45
HIGHEST = lax.Precision.HIGHEST

SUB = 8
LANES = 128
WIDE = 128
PART = 32
SLOTS = 4
RESIDENT_BYTES = 40 * 2**20
PART_ROWS = 16


def extra_rows(step):
    return 2 * SUB if step == 0 else SUB


F32 = jnp.float32
VMEM = pl.BlockSpec(memory_space=pltpu.VMEM)
HBM = pl.BlockSpec(memory_space=pltpu.HBM)
SMEM = pl.BlockSpec(memory_space=pltpu.SMEM)


def params(mib):
    return pltpu.CompilerParams(vmem_limit_bytes=mib * 2**20)


def tables(points):
    index = np.arange(points, dtype=np.int64) + 1
    momentum_step = CUTOFF / points
    radius_step = math.pi / ((points + 1) * momentum_step)
    sine = np.sin((index[:, None] * index[None, :]) % (2 * (points + 1)) * (math.pi / (points + 1)))
    momentum = index * momentum_step
    radius = index * radius_step
    forward = sine * (momentum[:, None] * momentum_step) / (2.0 * math.pi**2 * radius[None, :])
    backward = sine * (4.0 * math.pi * radius_step * radius[:, None]) / momentum[None, :]
    measure = momentum * momentum * momentum_step / (2.0 * math.pi**2)
    return tuple(np.asarray(a, np.float32) for a in (forward, backward, measure, momentum))


def shifts(size, amount):
    return [(i, (i + amount) % size) for i in range(size)]


def first_kernel(stat_hbm, spec_hbm, c0, c1, d0, d1, out_ref, stat_ref, spec_ref, sem):
    rows, _, width = stat_ref.shape
    latest = pl.ds(stat_hbm.shape[1] - SUB, SUB)
    copies = [
        pltpu.make_async_copy(stat_hbm.at[:, latest], stat_ref, sem.at[0]),
        pltpu.make_async_copy(spec_hbm.at[:, latest], spec_ref, sem.at[1]),
    ]
    for c in copies:
        c.start()
    for c in copies:
        c.wait()
    c0[...] = stat_ref[:, SUB - 2, :]
    c1[...] = stat_ref[:, SUB - 1, :]
    d0[...] = -spec_ref[:, SUB - 2, :]
    d1[...] = -spec_ref[:, SUB - 1, :]
    half = rows + SUB
    out_ref[0:rows, :] = c1[...]
    out_ref[half : half + rows, :] = d1[...]
    out_ref[rows:half, :] = jnp.zeros((SUB, width), F32)
    out_ref[half + rows :, :] = jnp.zeros((SUB, width), F32)


def load_kernel(counts, *refs):
    n = len(counts)
    sources, outs, sem = refs[:n], refs[n + 1 : 2 * n + 1], refs[-1]
    copies = [
        pltpu.make_async_copy(sources[i].at[pl.ds(start, count)], outs[i], sem.at[i])
        for i, (start, count) in enumerate(counts)
    ]
    for c in copies:
        c.start()
    for c in copies:
        c.wait()


def load(sources, counts, order):
    return pl.pallas_call(
        functools.partial(load_kernel, counts),
        out_shape=[pltpu.VMEM((n,) + s.shape[1:], F32) for s, (_, n) in zip(sources, counts)],
        in_specs=[HBM] * len(sources) + [VMEM],
        out_specs=[VMEM] * len(sources),
        scratch_shapes=[pltpu.SemaphoreType.DMA((len(sources),))],
        compiler_params=params(2),
        name="load",
    )(*sources, order)


def transform_kernel(step, blocks, *refs):
    current = step + 1
    place = refs[0]
    pieces = refs[1 : 1 + blocks]
    forward, backward, measure = refs[1 + blocks : 4 + blocks]
    stats = refs[4 + blocks : 5 + blocks + current]
    specs = refs[5 + blocks + current : 6 + blocks + 2 * current]
    out_ref, own_ref = refs[6 + blocks + 2 * current :]
    rows, width = stats[0].shape
    half = rows + SUB
    own = place[0]
    times = place[1] * rows
    radial = None
    tadpole = None
    for k in range(blocks):
        block = lax.rem(own + (blocks - k), blocks)
        part = jnp.dot(pieces[k][...], forward[block], precision=HIGHEST, preferred_element_type=F32)
        radial = part if radial is None else radial + part
        line = rows - 1 if step == 0 else rows + current
        part = jnp.sum(pieces[k][line : line + 1, :] * measure[block], axis=1, keepdims=True)
        tadpole = part if tadpole is None else tadpole + part
    stat = radial[:half]
    spec = radial[half:]
    square_stat = stat * stat
    square_spec = spec * spec
    sigma_stat = -SUNSET_COUPLING * stat * (square_stat - 0.75 * square_spec)
    sigma_spec = -SUNSET_COUPLING * spec * (3.0 * square_stat - 0.25 * square_spec)
    sigma = jnp.concatenate([sigma_stat, sigma_spec], axis=0)
    sigma = jnp.dot(sigma, backward[own], precision=HIGHEST, preferred_element_type=F32)
    group_stat = sigma[:rows]
    group_spec = sigma[half : half + rows]
    out_ref[0:rows, :] = group_stat
    out_ref[rows : 2 * rows, :] = group_spec
    own_ref[0:SUB, :] = sigma[rows:half]
    own_ref[SUB : 2 * SUB, :] = sigma[half + rows :]
    row_times = times + lax.broadcasted_iota(jnp.int32, (rows, width), 0)
    base = 2 * rows
    count = current + 1
    lines = []
    last = place[2]
    for a in range(count):
        later = row_times <= last - 1 + a
        partial = -group_spec * stats[a][...] - jnp.where(later, group_stat * specs[a][...], 0.0)
        lines.append(jnp.sum(partial, axis=0, keepdims=True))
    for a in range(2):
        earlier = row_times >= last - 1 + a
        partial = jnp.where(earlier, group_spec * specs[a][...], 0.0)
        lines.append(jnp.sum(partial, axis=0, keepdims=True))
    if step == 0:
        lines += [r[rows - 2 : rows, :] for r in (stats[0], stats[1], specs[0], specs[1])]
        lines.append(jnp.broadcast_to(tadpole, (1, width)))
    used = sum(v.shape[0] for v in lines)
    lines.append(jnp.zeros((extra_rows(step) - used, width), F32))
    out_ref[base:, :] = jnp.concatenate([v for v in lines if v.shape[0]], axis=0)
    own_ref[2 * SUB :, :] = jnp.broadcast_to(tadpole, (SUB, width))


def stack_kernel(count, *refs):
    out = refs[-1]
    for i in range(count):
        out[i] = refs[i][...]


def memory_kernel(step, group_sizes, resident, stream, *refs):
    current = step + 1
    newest = STEPS + 2
    hists, reps = group_sizes
    groups = hists * reps
    refs = list(refs)

    def take(n):
        head = refs[:n]
        del refs[:n]
        return head

    (place,) = take(1)
    firsts = take(reps)
    others = take(reps)
    (own_ref, momentum) = take(2)
    stats = take(current + 1)
    specs = take(current + 1)
    blocks_in = take(2) if step else None
    stat_parts = take(len(resident[0]))
    spec_parts = take(len(resident[1]))
    hbm = take(1) if stream else None
    last_step = step == STEPS - 1
    if last_step:
        rows_stat, rows_spec, block_stat, block_spec = take(4)
    else:
        next_stat_ref, next_spec_ref, block_stat, block_spec, out_ref = take(5)
    sig_stat, sig_spec, extra, mem_stat, mem_spec = take(5)
    if stream:
        buffers, sem = take(2)
    rows, width = stats[0].shape
    times = groups * rows
    hist, rep = place[3], place[4]
    group = hist * reps + rep
    chunks = rows // SUB

    parts = width // LANES
    units = (chunks - stream[0]) * parts if stream else 0

    def copy(unit):
        at = pl.multiple_of((stream[0] + unit // parts) * SUB, SUB)
        lane = pl.multiple_of((unit % parts) * LANES, LANES)
        source = hbm[0].at[pl.ds(at, SUB), :, pl.ds(lane, LANES)]
        return pltpu.make_async_copy(source, buffers.at[unit % SLOTS], sem.at[unit % SLOTS])

    for unit in range(min(SLOTS, units)):
        copy(jnp.int32(unit)).start()
    for k in range(hists):
        for q in range(reps):
            piece = firsts[q] if k == 0 else others[q].at[k - 1]
            who = lax.rem(hist + (hists - k), hists) * reps + lax.rem(rep + (reps - q), reps)
            at = pl.multiple_of(who * rows, SUB)
            sig_stat[pl.ds(at, rows), :] = piece[0:rows, :]
            sig_spec[pl.ds(at, rows), :] = piece[rows : 2 * rows, :]
            extra[who] = piece[2 * rows :, :]

    def find(parts, sizes, c):
        start = c * SUB
        for ref, (first, count) in zip(parts, sizes):
            if first <= start < first + count:
                return ref, start - first
        return None, 0

    for c in range(chunks):
        stat_ref, stat_at = find(stat_parts, resident[0], c)
        spec_ref, spec_at = find(spec_parts, resident[1], c)
        streamed = spec_ref is None

        def lanes(l, carry, c=c, stat_ref=stat_ref, stat_at=stat_at, spec_ref=spec_ref, spec_at=spec_at, streamed=streamed):
            first_time = group * rows + c * SUB
            middle = first_time // WIDE
            lane = pl.ds(pl.multiple_of(l * LANES, LANES), LANES)
            spec_lane = lane
            if streamed:
                unit = (c - stream[0]) * parts + l
                copy(unit).wait()
                spec_ref, spec_at = buffers.at[unit % SLOTS], 0
                spec_lane = pl.ds(0, LANES)

            def fold(value):
                return jnp.sum(value.reshape(PART // SUB, SUB, LANES), axis=0)

            def spans(j):
                return [pl.ds(pl.multiple_of(j * WIDE + p, PART), PART) for p in range(0, WIDE, PART)]

            def below(j, acc):
                acc_stat, acc_spec = list(acc[0]), list(acc[1])
                for at in spans(j):
                    weight_stat, weight_spec = sig_stat[at, lane], sig_spec[at, lane]
                    for r in range(SUB):
                        value = weight_spec * stat_ref[stat_at + r, at, lane]
                        acc_stat[r] += fold(value + weight_stat * spec_ref[spec_at + r, at, spec_lane])
                return tuple(acc_stat), tuple(acc_spec)

            def above(j, acc):
                acc_stat, acc_spec = list(acc[0]), list(acc[1])
                for at in spans(j):
                    weight_spec = sig_spec[at, lane]
                    for r in range(SUB):
                        acc_stat[r] += fold(weight_spec * stat_ref[stat_at + r, at, lane])
                        acc_spec[r] += fold(weight_spec * spec_ref[spec_at + r, at, spec_lane])
                return tuple(acc_stat), tuple(acc_spec)

            def around(j, acc):
                acc_stat, acc_spec = list(acc[0]), list(acc[1])
                index = j * WIDE - first_time + lax.broadcasted_iota(jnp.int32, (PART, LANES), 0)
                for p, at in enumerate(spans(j)):
                    weight_stat, weight_spec = sig_stat[at, lane], sig_spec[at, lane]
                    for r in range(SUB):
                        early = index <= r - p * PART
                        right = spec_ref[spec_at + r, at, spec_lane]
                        value = weight_spec * stat_ref[stat_at + r, at, lane]
                        acc_stat[r] += fold(value + jnp.where(early, weight_stat * right, 0.0))
                        acc_spec[r] += fold(jnp.where(early, 0.0, weight_spec * right))
                return tuple(acc_stat), tuple(acc_spec)

            none = jnp.zeros((SUB, LANES), F32)
            acc = (tuple(none for _ in range(SUB)), tuple(none for _ in range(SUB)))
            acc = lax.fori_loop(0, middle, below, acc)
            acc = around(middle, acc)
            acc = lax.fori_loop(middle + 1, times // WIDE, above, acc)
            here = pl.ds(c * SUB, SUB)
            mem_stat[here, lane] = -jnp.concatenate([jnp.sum(a, axis=0, keepdims=True) for a in acc[0]], axis=0)
            mem_spec[here, lane] = jnp.concatenate([jnp.sum(a, axis=0, keepdims=True) for a in acc[1]], axis=0)
            if streamed:

                @pl.when(unit + SLOTS < units)
                def _():
                    copy(unit + SLOTS).start()

            return carry

        lax.fori_loop(0, width // LANES, lanes, 0)

    factor = TIME_STEP * TIME_STEP
    corner = extra[groups - 1]
    index = lax.broadcasted_iota(jnp.int32, (SUB, width), 0)
    zero = jnp.zeros((SUB, width), F32)
    if step == 0:
        def pick(first, sign):
            out = []
            for a in range(2):
                left = corner[first + a : first + a + 1, :]
                right = corner[first + 2 + a : first + 3 + a, :]
                out.append(jnp.where(index == 0, sign * left, jnp.where(index == 1, sign * right, 0.0)))
            return out + [zero] * (newest - 2)

        blk_stat = pick(4, 1.0)
        blk_spec = pick(8, -1.0)
        tadpole = corner[12:13, :]
    else:
        blk_stat = [blocks_in[0][b] for b in range(newest)]
        blk_spec = [blocks_in[1][b] for b in range(newest)]
        tadpole = own_ref[2 * SUB : 2 * SUB + 1, :]
    momentum = momentum[place[0]]
    frequency = momentum * momentum + MASS_SQUARED + HARTREE_COUPLING * tadpole

    total = extra[0]
    for g in range(1, groups):
        total += extra[g]
    count = current + 1
    total_stat = jnp.concatenate([total[:count], jnp.zeros((SUB - count, width), F32)], axis=0)
    total_spec = jnp.concatenate([total[count : count + 2], jnp.zeros((SUB - 2, width), F32)], axis=0)
    memory_stat = mem_stat[...]
    memory_spec = mem_spec[...]
    for b in range(2, current + 1):
        weight_stat = own_ref[b : b + 1, :]
        weight_spec = own_ref[SUB + b : SUB + b + 1, :]
        memory_stat -= weight_spec * stats[b][...]
        memory_spec -= weight_spec * specs[b][...]
        total_stat -= weight_spec * blk_stat[b]
        total_stat += jnp.where(index >= b, weight_stat * blk_spec[b], 0.0)
        total_spec -= jnp.where(index <= b, weight_spec * blk_spec[b], 0.0)
    new_stat = (
        2.0 * stats[current][...]
        - stats[step][...]
        - factor * (frequency * stats[current][...] + TIME_STEP * memory_stat)
    )
    new_spec = (
        2.0 * specs[current][...]
        - specs[step][...]
        - factor * (frequency * specs[current][...] + TIME_STEP * memory_spec)
    )
    valid = index <= current
    line_stat = jnp.where(
        valid,
        2.0 * blk_stat[current]
        - blk_stat[step]
        - factor * (frequency * blk_stat[current] + TIME_STEP * total_stat),
        0.0,
    )
    line_spec = jnp.where(
        valid,
        2.0 * blk_spec[current]
        - blk_spec[step]
        - factor * (frequency * blk_spec[current] + TIME_STEP * total_spec),
        0.0,
    )
    diagonal = (
        2.0 * line_stat[current : current + 1]
        - line_stat[step : step + 1]
        - factor
        * (frequency * line_stat[current : current + 1] + TIME_STEP * total_stat[current : current + 1])
    )
    line_stat = jnp.where(index == current + 1, diagonal, line_stat)
    blk_stat[current + 1] = line_stat
    blk_spec[current + 1] = line_spec
    for b in range(newest):
        block_stat[b] = jnp.where(index == current + 1, line_stat[b : b + 1], blk_stat[b])
        block_spec[b] = jnp.where(index == current + 1, -line_spec[b : b + 1], blk_spec[b])
    if last_step:
        for b in range(2, newest - 1):
            rows_stat[b - 2] = stats[b][...]
            rows_spec[b - 2] = specs[b][...]
        rows_stat[newest - 3] = new_stat
        rows_spec[newest - 3] = new_spec
    else:
        next_stat_ref[...] = new_stat
        next_spec_ref[...] = new_spec
        half = rows + SUB
        out_ref[0:rows, :] = new_stat
        out_ref[half : half + rows, :] = new_spec
        out_ref[rows:half, :] = line_stat
        out_ref[half + rows :, :] = line_spec


def shards(history_stat, history_spec):
    rows, times, width = history_stat.shape
    history_stat = pltpu.with_memory_space_constraint(history_stat, pltpu.HBM)
    history_spec = pltpu.with_memory_space_constraint(history_spec, pltpu.HBM)
    newest = STEPS + 2
    half = rows + SUB
    hists, reps, moms = (lax.axis_size(a) for a in ("hist", "rep", "mom"))
    forward, backward, measure, momentum = tables(MOMENTA)
    forward = jnp.asarray(forward.reshape(moms, width, MOMENTA))
    backward = jnp.asarray(np.ascontiguousarray(backward.reshape(MOMENTA, moms, width).transpose(1, 0, 2)))
    measure = jnp.asarray(measure.reshape(moms, 1, width))
    own = lax.axis_index("mom")
    hist, rep = lax.axis_index("hist"), lax.axis_index("rep")
    momentum = jnp.asarray(momentum.reshape(moms, 1, width))
    place = jnp.stack([own, hist * reps + rep, jnp.int32(times - 1), hist, rep]).astype(jnp.int32)

    row_bytes = times * width * 4
    keep = min(2 * rows, RESIDENT_BYTES // row_bytes // SUB * SUB)
    keep_stat = rows
    keep_spec = keep - rows
    split = PART_ROWS
    sizes_stat = [(r, min(split, keep_stat - r)) for r in range(0, keep_stat, split)]
    sizes_spec = [(r, min(split, keep_spec - r)) for r in range(0, keep_spec, split)]
    stream = (keep_spec // SUB,) if keep_spec < rows else None

    c0, c1, d0, d1, send = pl.pallas_call(
        first_kernel,
        in_specs=[HBM] * 2,
        out_specs=[VMEM] * 5,
        out_shape=[jax.ShapeDtypeStruct((rows, width), F32)] * 4
        + [jax.ShapeDtypeStruct((2 * half, width), F32)],
        scratch_shapes=[pltpu.VMEM((rows, SUB, width), F32)] * 2 + [pltpu.SemaphoreType.DMA((2,))],
        compiler_params=params(3),
        name="first",
    )(history_stat, history_spec)
    stats, specs = [c0, c1], [d0, d1]
    blocks = ()
    for step in range(STEPS):
        pieces = [send]
        for k in range(1, moms):
            pieces.append(lax.ppermute(send, "mom", shifts(moms, k)))
        z, own_rows = pl.pallas_call(
            functools.partial(transform_kernel, step, moms),
            in_specs=[SMEM] + [VMEM] * (moms + 3 + len(stats) + len(specs)),
            out_specs=[VMEM] * 2,
            out_shape=[
                jax.ShapeDtypeStruct((2 * rows + extra_rows(step), width), F32),
                jax.ShapeDtypeStruct((3 * SUB, width), F32),
            ],
            compiler_params=params(6),
        )(place, *pieces, forward, backward, measure, *stats, *specs)
        along = []
        for k in range(1, hists):
            along.append(lax.ppermute(z, "hist", shifts(hists, k)))
        firsts = [z] + [lax.ppermute(z, "rep", shifts(reps, q)) for q in range(1, reps)]
        if step == 0:
            sources = [history_stat] * len(sizes_stat) + [history_spec] * len(sizes_spec)
            kept = []
            for source, count in zip(sources, sizes_stat + sizes_spec):
                kept += load([source], [count], z)
        other = pl.pallas_call(
            functools.partial(stack_kernel, hists - 1),
            in_specs=[VMEM] * (hists - 1),
            out_specs=VMEM,
            out_shape=jax.ShapeDtypeStruct((hists - 1,) + z.shape, F32),
            compiler_params=params(2),
            name="stack",
        )(*along)
        others = [other] + [lax.ppermute(other, "rep", shifts(reps, q)) for q in range(1, reps)]
        gathered = firsts + others
        last = step == STEPS - 1
        block_shape = jax.ShapeDtypeStruct((newest, SUB, width), F32)
        row_shape = jax.ShapeDtypeStruct((rows, width), F32)
        if last:
            out_shape = [jax.ShapeDtypeStruct((STEPS, rows, width), F32)] * 2 + [block_shape] * 2
        else:
            out_shape = [row_shape] * 2 + [block_shape] * 2
            out_shape += [jax.ShapeDtypeStruct((2 * half, width), F32)]
        scratch = [pltpu.VMEM((times, width), F32)] * 2 + [
            pltpu.VMEM((hists * reps, extra_rows(step), width), F32),
            pltpu.VMEM((rows, width), F32),
            pltpu.VMEM((rows, width), F32),
        ]
        operands = [*gathered, own_rows, momentum, *stats, *specs, *blocks, *kept]
        in_specs = [SMEM] + [VMEM] * len(operands)
        if stream:
            operands.append(history_spec)
            in_specs.append(HBM)
            scratch += [pltpu.VMEM((SLOTS, SUB, times, LANES), F32), pltpu.SemaphoreType.DMA((SLOTS,))]
        outs = pl.pallas_call(
            functools.partial(
                memory_kernel, step, (hists, reps), (sizes_stat, sizes_spec), stream
            ),
            in_specs=in_specs,
            out_specs=[VMEM] * len(out_shape),
            out_shape=out_shape,
            scratch_shapes=scratch,
            compiler_params=params(11),
        )(place, *operands)
        if last:
            return outs[0], outs[1], outs[2][:, :newest], outs[3][:, :newest]
        stats.append(outs[0])
        specs.append(outs[1])
        blocks = (outs[2], outs[3])
        send = outs[4]


def solution(mesh):
    in_specs = (P(("hist", "rep"), "ens", "mom"), P(("hist", "rep"), "ens", "mom"))
    out_specs = (
        P("ens", ("hist", "rep"), "mom"),
        P("ens", ("hist", "rep"), "mom"),
        P("ens", None, "mom"),
        P("ens", None, "mom"),
    )
    return jax.shard_map(shards, mesh=mesh, in_specs=in_specs, out_specs=out_specs, check_vma=False)
```

```python
import functools
import math

import jax
import jax.numpy as jnp
import numpy as np
from jax import lax
from jax.experimental import pallas as pl
from jax.experimental.pallas import tpu as pltpu
from jax.sharding import PartitionSpec as P


MOMENTA = 512
STEPS = 3
TIME_STEP = 0.12
CUTOFF = 12.8
MASS_SQUARED = 1.0
SUNSET_COUPLING = 100.0
HARTREE_COUPLING = 2.45
BF16 = np.dtype(jnp.bfloat16)

SUB = 8
LANES = 128
WIDE = 128
PART = 32
SLOTS = 4
RESIDENT_BYTES = 40 * 2**20
PART_ROWS = 16


def extra_rows(step):
    return 2 * SUB if step == 0 else SUB


F32 = jnp.float32
VMEM = pl.BlockSpec(memory_space=pltpu.VMEM)
HBM = pl.BlockSpec(memory_space=pltpu.HBM)
SMEM = pl.BlockSpec(memory_space=pltpu.SMEM)


def params(mib):
    return pltpu.CompilerParams(vmem_limit_bytes=mib * 2**20)


def tables(points):
    index = np.arange(points, dtype=np.int64) + 1
    momentum_step = CUTOFF / points
    radius_step = math.pi / ((points + 1) * momentum_step)
    sine = np.sin((index[:, None] * index[None, :]) % (2 * (points + 1)) * (math.pi / (points + 1)))
    momentum = index * momentum_step
    radius = index * radius_step
    forward = sine * (momentum[:, None] * momentum_step) / (2.0 * math.pi**2 * radius[None, :])
    backward = sine * (4.0 * math.pi * radius_step * radius[:, None]) / momentum[None, :]
    measure = momentum * momentum * momentum_step / (2.0 * math.pi**2)
    return tuple(np.asarray(a, np.float32) for a in (forward, backward, measure, momentum))


def split(table):
    high = table.astype(BF16)
    return jnp.asarray(np.stack([high, (table - high.astype(np.float32)).astype(BF16)], axis=1))


def product(value, table):
    high = value.astype(jnp.bfloat16)
    low = (value - high.astype(F32)).astype(jnp.bfloat16)

    def dot(a, b):
        return jnp.dot(a, b, preferred_element_type=F32)

    return dot(high, table[0]) + (dot(high, table[1]) + dot(low, table[0]))


def shifts(size, amount):
    return [(i, (i + amount) % size) for i in range(size)]


def first_kernel(stat_hbm, spec_hbm, c0, c1, d0, d1, out_ref, stat_ref, spec_ref, sem):
    rows, _, width = stat_ref.shape
    latest = pl.ds(stat_hbm.shape[1] - SUB, SUB)
    copies = [
        pltpu.make_async_copy(stat_hbm.at[:, latest], stat_ref, sem.at[0]),
        pltpu.make_async_copy(spec_hbm.at[:, latest], spec_ref, sem.at[1]),
    ]
    for c in copies:
        c.start()
    for c in copies:
        c.wait()
    c0[...] = stat_ref[:, SUB - 2, :]
    c1[...] = stat_ref[:, SUB - 1, :]
    d0[...] = -spec_ref[:, SUB - 2, :]
    d1[...] = -spec_ref[:, SUB - 1, :]
    half = rows + SUB
    out_ref[0:rows, :] = c1[...]
    out_ref[half : half + rows, :] = d1[...]
    out_ref[rows:half, :] = jnp.zeros((SUB, width), F32)
    out_ref[half + rows :, :] = jnp.zeros((SUB, width), F32)


def load_kernel(counts, *refs):
    n = len(counts)
    sources, outs, sem = refs[:n], refs[n + 1 : 2 * n + 1], refs[-1]
    copies = [
        pltpu.make_async_copy(sources[i].at[pl.ds(start, count)], outs[i], sem.at[i])
        for i, (start, count) in enumerate(counts)
    ]
    for c in copies:
        c.start()
    for c in copies:
        c.wait()


def load(sources, counts, order):
    return pl.pallas_call(
        functools.partial(load_kernel, counts),
        out_shape=[pltpu.VMEM((n,) + s.shape[1:], F32) for s, (_, n) in zip(sources, counts)],
        in_specs=[HBM] * len(sources) + [VMEM],
        out_specs=[VMEM] * len(sources),
        scratch_shapes=[pltpu.SemaphoreType.DMA((len(sources),))],
        compiler_params=params(2),
        name="load",
    )(*sources, order)


def transform_kernel(step, blocks, *refs):
    current = step + 1
    place = refs[0]
    pieces = refs[1 : 1 + blocks]
    forward, backward, measure = refs[1 + blocks : 4 + blocks]
    stats = refs[4 + blocks : 5 + blocks + current]
    specs = refs[5 + blocks + current : 6 + blocks + 2 * current]
    out_ref, own_ref = refs[6 + blocks + 2 * current :]
    rows, width = stats[0].shape
    half = rows + SUB
    own = place[0]
    times = place[1] * rows
    radial = None
    tadpole = None
    for k in range(blocks):
        block = lax.rem(own + (blocks - k), blocks)
        part = product(pieces[k][...], forward[block])
        radial = part if radial is None else radial + part
        line = rows - 1 if step == 0 else rows + current
        part = jnp.sum(pieces[k][line : line + 1, :] * measure[block], axis=1, keepdims=True)
        tadpole = part if tadpole is None else tadpole + part
    stat = radial[:half]
    spec = radial[half:]
    square_stat = stat * stat
    square_spec = spec * spec
    sigma_stat = -SUNSET_COUPLING * stat * (square_stat - 0.75 * square_spec)
    sigma_spec = -SUNSET_COUPLING * spec * (3.0 * square_stat - 0.25 * square_spec)
    sigma = jnp.concatenate([sigma_stat, sigma_spec], axis=0)
    sigma = product(sigma, backward[own])
    group_stat = sigma[:rows]
    group_spec = sigma[half : half + rows]
    out_ref[0:rows, :] = group_stat
    out_ref[rows : 2 * rows, :] = group_spec
    own_ref[0:SUB, :] = sigma[rows:half]
    own_ref[SUB : 2 * SUB, :] = sigma[half + rows :]
    row_times = times + lax.broadcasted_iota(jnp.int32, (rows, width), 0)
    base = 2 * rows
    count = current + 1
    lines = []
    last = place[2]
    for a in range(count):
        later = row_times <= last - 1 + a
        partial = -group_spec * stats[a][...] - jnp.where(later, group_stat * specs[a][...], 0.0)
        lines.append(jnp.sum(partial, axis=0, keepdims=True))
    for a in range(2):
        earlier = row_times >= last - 1 + a
        partial = jnp.where(earlier, group_spec * specs[a][...], 0.0)
        lines.append(jnp.sum(partial, axis=0, keepdims=True))
    if step == 0:
        lines += [r[rows - 2 : rows, :] for r in (stats[0], stats[1], specs[0], specs[1])]
        lines.append(jnp.broadcast_to(tadpole, (1, width)))
    used = sum(v.shape[0] for v in lines)
    lines.append(jnp.zeros((extra_rows(step) - used, width), F32))
    out_ref[base:, :] = jnp.concatenate([v for v in lines if v.shape[0]], axis=0)
    own_ref[2 * SUB :, :] = jnp.broadcast_to(tadpole, (SUB, width))


def stack_kernel(count, *refs):
    out = refs[-1]
    for i in range(count):
        out[i] = refs[i][...]


def memory_kernel(step, group_sizes, resident, stream, *refs):
    current = step + 1
    newest = STEPS + 2
    hists, reps = group_sizes
    groups = hists * reps
    refs = list(refs)

    def take(n):
        head = refs[:n]
        del refs[:n]
        return head

    (place,) = take(1)
    firsts = take(reps)
    others = take(reps)
    (own_ref, momentum) = take(2)
    stats = take(current + 1)
    specs = take(current + 1)
    blocks_in = take(2) if step else None
    stat_parts = take(len(resident[0]))
    spec_parts = take(len(resident[1]))
    hbm = take(1) if stream else None
    last_step = step == STEPS - 1
    if last_step:
        rows_stat, rows_spec, block_stat, block_spec = take(4)
    else:
        next_stat_ref, next_spec_ref, block_stat, block_spec, out_ref = take(5)
    sig_stat, sig_spec, extra, mem_stat, mem_spec = take(5)
    if stream:
        buffers, sem = take(2)
    rows, width = stats[0].shape
    times = groups * rows
    hist, rep = place[3], place[4]
    group = hist * reps + rep
    chunks = rows // SUB

    parts = width // LANES
    units = (chunks - stream[0]) * parts if stream else 0

    def copy(unit):
        at = pl.multiple_of((stream[0] + unit // parts) * SUB, SUB)
        lane = pl.multiple_of((unit % parts) * LANES, LANES)
        source = hbm[0].at[pl.ds(at, SUB), :, pl.ds(lane, LANES)]
        return pltpu.make_async_copy(source, buffers.at[unit % SLOTS], sem.at[unit % SLOTS])

    for unit in range(min(SLOTS, units)):
        copy(jnp.int32(unit)).start()
    for k in range(hists):
        for q in range(reps):
            piece = firsts[q] if k == 0 else others[q].at[k - 1]
            who = lax.rem(hist + (hists - k), hists) * reps + lax.rem(rep + (reps - q), reps)
            at = pl.multiple_of(who * rows, SUB)
            sig_stat[pl.ds(at, rows), :] = piece[0:rows, :]
            sig_spec[pl.ds(at, rows), :] = piece[rows : 2 * rows, :]
            extra[who] = piece[2 * rows :, :]

    def find(parts, sizes, c):
        start = c * SUB
        for ref, (first, count) in zip(parts, sizes):
            if first <= start < first + count:
                return ref, start - first
        return None, 0

    for c in range(chunks):
        stat_ref, stat_at = find(stat_parts, resident[0], c)
        spec_ref, spec_at = find(spec_parts, resident[1], c)
        streamed = spec_ref is None

        def lanes(l, carry, c=c, stat_ref=stat_ref, stat_at=stat_at, spec_ref=spec_ref, spec_at=spec_at, streamed=streamed):
            first_time = group * rows + c * SUB
            middle = first_time // WIDE
            lane = pl.ds(pl.multiple_of(l * LANES, LANES), LANES)
            spec_lane = lane
            if streamed:
                unit = (c - stream[0]) * parts + l
                copy(unit).wait()
                spec_ref, spec_at = buffers.at[unit % SLOTS], 0
                spec_lane = pl.ds(0, LANES)

            def fold(value):
                return jnp.sum(value.reshape(PART // SUB, SUB, LANES), axis=0)

            def spans(j):
                return [pl.ds(pl.multiple_of(j * WIDE + p, PART), PART) for p in range(0, WIDE, PART)]

            def below(j, acc):
                acc_stat, acc_spec = list(acc[0]), list(acc[1])
                for at in spans(j):
                    weight_stat, weight_spec = sig_stat[at, lane], sig_spec[at, lane]
                    for r in range(SUB):
                        value = weight_spec * stat_ref[stat_at + r, at, lane]
                        acc_stat[r] += fold(value + weight_stat * spec_ref[spec_at + r, at, spec_lane])
                return tuple(acc_stat), tuple(acc_spec)

            def above(j, acc):
                acc_stat, acc_spec = list(acc[0]), list(acc[1])
                for at in spans(j):
                    weight_spec = sig_spec[at, lane]
                    for r in range(SUB):
                        acc_stat[r] += fold(weight_spec * stat_ref[stat_at + r, at, lane])
                        acc_spec[r] += fold(weight_spec * spec_ref[spec_at + r, at, spec_lane])
                return tuple(acc_stat), tuple(acc_spec)

            def around(j, acc):
                acc_stat, acc_spec = list(acc[0]), list(acc[1])
                index = j * WIDE - first_time + lax.broadcasted_iota(jnp.int32, (PART, LANES), 0)
                for p, at in enumerate(spans(j)):
                    weight_stat, weight_spec = sig_stat[at, lane], sig_spec[at, lane]
                    for r in range(SUB):
                        early = index <= r - p * PART
                        right = spec_ref[spec_at + r, at, spec_lane]
                        value = weight_spec * stat_ref[stat_at + r, at, lane]
                        acc_stat[r] += fold(value + jnp.where(early, weight_stat * right, 0.0))
                        acc_spec[r] += fold(jnp.where(early, 0.0, weight_spec * right))
                return tuple(acc_stat), tuple(acc_spec)

            none = jnp.zeros((SUB, LANES), F32)
            acc = (tuple(none for _ in range(SUB)), tuple(none for _ in range(SUB)))
            acc = lax.fori_loop(0, middle, below, acc)
            acc = around(middle, acc)
            acc = lax.fori_loop(middle + 1, times // WIDE, above, acc)
            here = pl.ds(c * SUB, SUB)
            mem_stat[here, lane] = -jnp.concatenate([jnp.sum(a, axis=0, keepdims=True) for a in acc[0]], axis=0)
            mem_spec[here, lane] = jnp.concatenate([jnp.sum(a, axis=0, keepdims=True) for a in acc[1]], axis=0)
            if streamed:

                @pl.when(unit + SLOTS < units)
                def _():
                    copy(unit + SLOTS).start()

            return carry

        lax.fori_loop(0, width // LANES, lanes, 0)

    factor = TIME_STEP * TIME_STEP
    corner = extra[groups - 1]
    index = lax.broadcasted_iota(jnp.int32, (SUB, width), 0)
    zero = jnp.zeros((SUB, width), F32)
    if step == 0:
        def pick(first, sign):
            out = []
            for a in range(2):
                left = corner[first + a : first + a + 1, :]
                right = corner[first + 2 + a : first + 3 + a, :]
                out.append(jnp.where(index == 0, sign * left, jnp.where(index == 1, sign * right, 0.0)))
            return out + [zero] * (newest - 2)

        blk_stat = pick(4, 1.0)
        blk_spec = pick(8, -1.0)
        tadpole = corner[12:13, :]
    else:
        blk_stat = [blocks_in[0][b] for b in range(newest)]
        blk_spec = [blocks_in[1][b] for b in range(newest)]
        tadpole = own_ref[2 * SUB : 2 * SUB + 1, :]
    momentum = momentum[place[0]]
    frequency = momentum * momentum + MASS_SQUARED + HARTREE_COUPLING * tadpole

    total = extra[0]
    for g in range(1, groups):
        total += extra[g]
    count = current + 1
    total_stat = jnp.concatenate([total[:count], jnp.zeros((SUB - count, width), F32)], axis=0)
    total_spec = jnp.concatenate([total[count : count + 2], jnp.zeros((SUB - 2, width), F32)], axis=0)
    memory_stat = mem_stat[...]
    memory_spec = mem_spec[...]
    for b in range(2, current + 1):
        weight_stat = own_ref[b : b + 1, :]
        weight_spec = own_ref[SUB + b : SUB + b + 1, :]
        memory_stat -= weight_spec * stats[b][...]
        memory_spec -= weight_spec * specs[b][...]
        total_stat -= weight_spec * blk_stat[b]
        total_stat += jnp.where(index >= b, weight_stat * blk_spec[b], 0.0)
        total_spec -= jnp.where(index <= b, weight_spec * blk_spec[b], 0.0)
    new_stat = (
        2.0 * stats[current][...]
        - stats[step][...]
        - factor * (frequency * stats[current][...] + TIME_STEP * memory_stat)
    )
    new_spec = (
        2.0 * specs[current][...]
        - specs[step][...]
        - factor * (frequency * specs[current][...] + TIME_STEP * memory_spec)
    )
    valid = index <= current
    line_stat = jnp.where(
        valid,
        2.0 * blk_stat[current]
        - blk_stat[step]
        - factor * (frequency * blk_stat[current] + TIME_STEP * total_stat),
        0.0,
    )
    line_spec = jnp.where(
        valid,
        2.0 * blk_spec[current]
        - blk_spec[step]
        - factor * (frequency * blk_spec[current] + TIME_STEP * total_spec),
        0.0,
    )
    diagonal = (
        2.0 * line_stat[current : current + 1]
        - line_stat[step : step + 1]
        - factor
        * (frequency * line_stat[current : current + 1] + TIME_STEP * total_stat[current : current + 1])
    )
    line_stat = jnp.where(index == current + 1, diagonal, line_stat)
    blk_stat[current + 1] = line_stat
    blk_spec[current + 1] = line_spec
    for b in range(newest):
        block_stat[b] = jnp.where(index == current + 1, line_stat[b : b + 1], blk_stat[b])
        block_spec[b] = jnp.where(index == current + 1, -line_spec[b : b + 1], blk_spec[b])
    if last_step:
        for b in range(2, newest - 1):
            rows_stat[b - 2] = stats[b][...]
            rows_spec[b - 2] = specs[b][...]
        rows_stat[newest - 3] = new_stat
        rows_spec[newest - 3] = new_spec
    else:
        next_stat_ref[...] = new_stat
        next_spec_ref[...] = new_spec
        half = rows + SUB
        out_ref[0:rows, :] = new_stat
        out_ref[half : half + rows, :] = new_spec
        out_ref[rows:half, :] = line_stat
        out_ref[half + rows :, :] = line_spec


def shards(history_stat, history_spec):
    rows, times, width = history_stat.shape
    history_stat = pltpu.with_memory_space_constraint(history_stat, pltpu.HBM)
    history_spec = pltpu.with_memory_space_constraint(history_spec, pltpu.HBM)
    newest = STEPS + 2
    half = rows + SUB
    hists, reps, moms = (lax.axis_size(a) for a in ("hist", "rep", "mom"))
    forward, backward, measure, momentum = tables(MOMENTA)
    forward = split(forward.reshape(moms, width, MOMENTA))
    backward = split(np.ascontiguousarray(backward.reshape(MOMENTA, moms, width).transpose(1, 0, 2)))
    measure = jnp.asarray(measure.reshape(moms, 1, width))
    own = lax.axis_index("mom")
    hist, rep = lax.axis_index("hist"), lax.axis_index("rep")
    momentum = jnp.asarray(momentum.reshape(moms, 1, width))
    place = jnp.stack([own, hist * reps + rep, jnp.int32(times - 1), hist, rep]).astype(jnp.int32)

    row_bytes = times * width * 4
    keep = min(2 * rows, RESIDENT_BYTES // row_bytes // SUB * SUB)
    keep_stat = rows
    keep_spec = keep - rows
    part = PART_ROWS
    sizes_stat = [(r, min(part, keep_stat - r)) for r in range(0, keep_stat, part)]
    sizes_spec = [(r, min(part, keep_spec - r)) for r in range(0, keep_spec, part)]
    stream = (keep_spec // SUB,) if keep_spec < rows else None

    c0, c1, d0, d1, send = pl.pallas_call(
        first_kernel,
        in_specs=[HBM] * 2,
        out_specs=[VMEM] * 5,
        out_shape=[jax.ShapeDtypeStruct((rows, width), F32)] * 4
        + [jax.ShapeDtypeStruct((2 * half, width), F32)],
        scratch_shapes=[pltpu.VMEM((rows, SUB, width), F32)] * 2 + [pltpu.SemaphoreType.DMA((2,))],
        compiler_params=params(3),
        name="first",
    )(history_stat, history_spec)
    stats, specs = [c0, c1], [d0, d1]
    blocks = ()
    for step in range(STEPS):
        pieces = [send]
        for k in range(1, moms):
            pieces.append(lax.ppermute(send, "mom", shifts(moms, k)))
        z, own_rows = pl.pallas_call(
            functools.partial(transform_kernel, step, moms),
            in_specs=[SMEM] + [VMEM] * (moms + 3 + len(stats) + len(specs)),
            out_specs=[VMEM] * 2,
            out_shape=[
                jax.ShapeDtypeStruct((2 * rows + extra_rows(step), width), F32),
                jax.ShapeDtypeStruct((3 * SUB, width), F32),
            ],
            compiler_params=params(6),
        )(place, *pieces, forward, backward, measure, *stats, *specs)
        along = []
        for k in range(1, hists):
            along.append(lax.ppermute(z, "hist", shifts(hists, k)))
        firsts = [z] + [lax.ppermute(z, "rep", shifts(reps, q)) for q in range(1, reps)]
        if step == 0:
            sources = [history_stat] * len(sizes_stat) + [history_spec] * len(sizes_spec)
            kept = []
            for source, count in zip(sources, sizes_stat + sizes_spec):
                kept += load([source], [count], z)
        other = pl.pallas_call(
            functools.partial(stack_kernel, hists - 1),
            in_specs=[VMEM] * (hists - 1),
            out_specs=VMEM,
            out_shape=jax.ShapeDtypeStruct((hists - 1,) + z.shape, F32),
            compiler_params=params(2),
            name="stack",
        )(*along)
        others = [other] + [lax.ppermute(other, "rep", shifts(reps, q)) for q in range(1, reps)]
        gathered = firsts + others
        last = step == STEPS - 1
        block_shape = jax.ShapeDtypeStruct((newest, SUB, width), F32)
        row_shape = jax.ShapeDtypeStruct((rows, width), F32)
        if last:
            out_shape = [jax.ShapeDtypeStruct((STEPS, rows, width), F32)] * 2 + [block_shape] * 2
        else:
            out_shape = [row_shape] * 2 + [block_shape] * 2
            out_shape += [jax.ShapeDtypeStruct((2 * half, width), F32)]
        scratch = [pltpu.VMEM((times, width), F32)] * 2 + [
            pltpu.VMEM((hists * reps, extra_rows(step), width), F32),
            pltpu.VMEM((rows, width), F32),
            pltpu.VMEM((rows, width), F32),
        ]
        operands = [*gathered, own_rows, momentum, *stats, *specs, *blocks, *kept]
        in_specs = [SMEM] + [VMEM] * len(operands)
        if stream:
            operands.append(history_spec)
            in_specs.append(HBM)
            scratch += [pltpu.VMEM((SLOTS, SUB, times, LANES), F32), pltpu.SemaphoreType.DMA((SLOTS,))]
        outs = pl.pallas_call(
            functools.partial(
                memory_kernel, step, (hists, reps), (sizes_stat, sizes_spec), stream
            ),
            in_specs=in_specs,
            out_specs=[VMEM] * len(out_shape),
            out_shape=out_shape,
            scratch_shapes=scratch,
            compiler_params=params(11),
        )(place, *operands)
        if last:
            return outs[0], outs[1], outs[2][:, :newest], outs[3][:, :newest]
        stats.append(outs[0])
        specs.append(outs[1])
        blocks = (outs[2], outs[3])
        send = outs[4]


def solution(mesh):
    in_specs = (P(("hist", "rep"), "ens", "mom"), P(("hist", "rep"), "ens", "mom"))
    out_specs = (
        P("ens", ("hist", "rep"), "mom"),
        P("ens", ("hist", "rep"), "mom"),
        P("ens", None, "mom"),
        P("ens", None, "mom"),
    )
    return jax.shard_map(shards, mesh=mesh, in_specs=in_specs, out_specs=out_specs, check_vma=False)
```
